32 devices in a mesh: gx: 8 (over z, y), gy: 4 (over x, core).
Axes of the slice: x: 2, y: 2, z: 4, core: 2. Of those that a mesh axis runs over, the one named last changes fastest.
Arguments:
- tokens: bfloat16 [256, 8192], P('gy', 'gx'), may hold values from -6 to 6
- target: bfloat16 [256, 8192], P('gy', 'gx'), may hold values from -6 to 6
- w_gate: bfloat16 [8192, 14336], P('gx', 'gy'), may hold values from -0.0625 to 0.0625
- w_up: bfloat16 [8192, 14336], P('gx', 'gy'), may hold values from -0.0625 to 0.0625
- w_down: bfloat16 [14336, 8192], P('gy', 'gx'), may hold values from -0.046875 to 0.046875
- t_gate: bfloat16 [8192, 14336], P('gx', 'gy'), may hold values from -0.0625 to 0.0625
- t_up: bfloat16 [8192, 14336], P('gx', 'gy'), may hold values from -0.0625 to 0.0625
- t_down: bfloat16 [14336, 8192], P('gy', 'gx'), may hold values from -0.046875 to 0.046875
Outputs:
- hvp_gate: bfloat16 [8192, 14336], P('gx', 'gy')
- hvp_up: bfloat16 [8192, 14336], P('gx', 'gy')
- hvp_down: bfloat16 [14336, 8192], P('gy', 'gx')
The draws below stay inside these ranges and needn't reach their ends.
All inputs are finite; a program needn't handle non-finite values.
Results may differ from the reference program's by a relative error of at most 0.0074.
Values may be sent and summed in bfloat16 or wider, within the bound.
No kernel may reach another device: no remote copies, remote signals or barrier semaphores. Data moves between devices by JAX's collectives and lax.ppermute only.
A program may use at most 192 MiB of HBM per device.

```python
import math
import jax
import jax.numpy as jnp

D = 8192
FF = 14336
TOKENS = 256


def spiked(drawn, rng, source, target, blocks, factor):
    def block_of(position):
        return (jnp.arange(drawn.shape[position]) // (drawn.shape[position] // blocks)).reshape((-1,) + (1,) * (drawn.ndim - 1 - position))

    near = jax.random.permutation(rng, blocks)[block_of(target)]
    other_side = (block_of(target) + blocks // 2) % blocks
    return jnp.where((block_of(source) == near) | (block_of(source) == other_side), factor * drawn, drawn)


def levels(rng, extent, split, smallest, high):
    factor_of = 1.0
    for axis_at, parts in split:
        draws = jax.random.uniform(jax.random.fold_in(jax.random.fold_in(rng, 6), axis_at), (parts,), jnp.float32, smallest / len(split), high / len(split))
        factor_of = factor_of * jnp.repeat(jnp.exp(draws), extent[axis_at] // parts).reshape((-1,) + (1,) * (len(extent) - 1 - axis_at))
    return factor_of


def centred(own_key, extent, deviation, most, split=(), held_as=jnp.bfloat16):
    loudness = levels(own_key, extent, split, -0.22, 0.18) if split else 1.0
    result = jax.random.normal(own_key, extent, jnp.float32) * deviation * loudness
    return jnp.minimum(jnp.maximum(result, -most), most).astype(held_as)


def heavy_noise(stream_key, shape, spread, limit, shards, heavy, kind=jnp.bfloat16):
    array = spread * jax.random.normal(stream_key, shape, jnp.float32)
    if shards:
        array = array * levels(stream_key, shape, shards, -0.22, 0.18)
    return jnp.clip(spiked(array, jax.random.fold_in(stream_key, 3), *heavy), -limit, limit).astype(kind)


def setup_inputs(seed: int = 0) -> dict:
    key_of = jax.random.split(jax.random.key(seed), 9)
    tokens = heavy_noise(key_of[0], (TOKENS, D), 1.0, 6.0, ((0, 4), (1, 8)), (1, 0, 8, 2.0))
    target = centred(key_of[1], (TOKENS, D), 1.0, 6.0, ((0, 4), (1, 8)))
    w_gate = centred(key_of[2], (D, FF), D ** -0.5, 0.0625, ((0, 8), (1, 4)))
    w_up = centred(key_of[3], (D, FF), D ** -0.5, 0.0625, ((0, 8), (1, 4)))
    w_down = centred(key_of[4], (FF, D), FF ** -0.5, 0.046875, ((0, 4), (1, 8)))
    t_gate = centred(key_of[5], (D, FF), D ** -0.5, 0.0625, ((0, 8), (1, 4)))
    t_up = centred(key_of[6], (D, FF), D ** -0.5, 0.0625, ((0, 8), (1, 4)))
    t_down = centred(key_of[7], (FF, D), FF ** -0.5, 0.046875, ((0, 4), (1, 8)))
    return {"tokens": tokens, "target": target, "w_gate": w_gate, "w_up": w_up, "w_down": w_down, "t_gate": t_gate, "t_up": t_up, "t_down": t_down}


def silu_parts(gate):
    sig = jax.nn.sigmoid(gate)
    first = sig * (1.0 + gate * (1.0 - sig))
    second = sig * (1.0 - sig) * (2.0 + gate * (1.0 - 2.0 * sig))
    return (gate * sig, first, second)

def matmul(left, right):
    return jnp.dot(left, right, preferred_element_type=jnp.float32)

def reference(tokens, target, w_gate, w_up, w_down, t_gate, t_up, t_down):
    scale = 1.0 / math.sqrt(TOKENS)
    gate = matmul(tokens, w_gate)
    upper = matmul(tokens, w_up)
    gate_dot = matmul(tokens, t_gate)
    upper_dot = matmul(tokens, t_up)
    silu_val, first, second = silu_parts(gate)
    hidden = (silu_val * upper).astype(jnp.bfloat16)
    hidden_dot = (first * gate_dot * upper + silu_val * upper_dot).astype(jnp.bfloat16)
    output = matmul(hidden, w_down)
    output_dot = matmul(hidden_dot, w_down) + matmul(hidden, t_down)
    grad = ((output - target.astype(jnp.float32)) * scale).astype(jnp.bfloat16)
    grad_dot = (output_dot * scale).astype(jnp.bfloat16)
    hvp_down = (matmul(hidden_dot.T, grad) + matmul(hidden.T, grad_dot)).astype(jnp.bfloat16)
    back = matmul(grad, w_down.T)
    back_dot = matmul(grad_dot, w_down.T) + matmul(grad, t_down.T)
    gate_in = (back_dot * upper * first + back * upper_dot * first + back * upper * second * gate_dot).astype(jnp.bfloat16)
    upper_in = (back_dot * silu_val + back * first * gate_dot).astype(jnp.bfloat16)
    hvp_gate = matmul(tokens.T, gate_in).astype(jnp.bfloat16)
    hvp_up = matmul(tokens.T, upper_in).astype(jnp.bfloat16)
    return (hvp_gate, hvp_up, hvp_down)
```

```python
import math

import jax
import jax.numpy as jnp
from jax import lax
from jax.sharding import PartitionSpec as P

LANES = 128
BF16 = jnp.bfloat16
F32 = jnp.float32


def silu_parts(gate):
    sig = jax.nn.sigmoid(gate)
    first = sig * (1.0 + gate * (1.0 - sig))
    second = sig * (1.0 - sig) * (2.0 + gate * (1.0 - 2.0 * sig))
    return (gate * sig, first, second)


def matmul(left, right):
    return jnp.dot(left, right, preferred_element_type=F32)


def lead_dot(left, right):
    return lax.dot_general(left, right, (((0,), (0,)), ((), ())), preferred_element_type=F32)


def tail_dot(left, right):
    return lax.dot_general(left, right, (((1,), (1,)), ((), ())), preferred_element_type=F32)


class Ring:
    def __init__(self, size, tokens, width):
        self.size = size
        self.half = size // 2
        order = list(range(0, size, 2)) + list(range(size - 1, 0, -2))
        self.ahead = [(order[k], order[(k + 1) % size]) for k in range(size)]
        self.back = [(b, a) for a, b in self.ahead]
        index = lax.axis_index("gx")
        self.pos = jnp.where(index % 2 == 0, index // 2, size - 1 - index // 2)
        self.cols = max(c for c in range(1, size) if size % c == 0 and width % (c * LANES) == 0)
        self.parts = size // self.cols
        self.rows = tokens // self.parts
        self.width = width // self.cols

    def column(self, offset):
        return lax.rem(self.pos + offset + self.size, self.cols)

    def row_part(self, offset):
        return lax.rem(self.pos + offset + self.size, self.size) // self.cols

    def rows_of(self, array, offset):
        return lax.dynamic_slice_in_dim(array, self.row_part(offset) * self.rows, self.rows, 0)

    def reduce_scatter(self, own):
        flying = {}
        for far in range(self.half, 0, -1):
            for way in (1, -1):
                for piece in (0, 1):
                    first = (way == 1) == (piece == 0)
                    if far == self.half and not first:
                        continue
                    value = own(way * far, piece)
                    if (way, piece) in flying:
                        value = value + flying[way, piece].astype(F32)
                    flying[way, piece] = lax.ppermute(
                        value.astype(BF16), "gx", self.ahead if way == 1 else self.back
                    )
        return [
            own(0, piece) + flying[1, piece].astype(F32) + flying[-1, piece].astype(F32)
            for piece in (0, 1)
        ]

    def all_gather(self, mine, use):
        held = {0: list(mine)}
        flying = {(way, piece): mine[piece] for way in (1, -1) for piece in (0, 1)}
        waiting = set(range(self.cols))
        for far in range(0, self.half + 1):
            if far:
                for way in (1, -1):
                    for piece in (0, 1):
                        if far == self.half and (way == 1) != (piece == 0):
                            continue
                        got = lax.ppermute(
                            flying[way, piece], "gx", self.ahead if way == 1 else self.back
                        )
                        flying[way, piece] = got
                        offset = self.half if far == self.half else -way * far
                        held.setdefault(offset, [None, None])[piece] = got
            for part in sorted(waiting):
                offsets = [o for o in range(1 - self.half, self.half + 1) if (o - part) % self.cols == 0]
                if all(o in held for o in offsets):
                    waiting.discard(part)
                    use(part, [self.in_order(offsets, [held[o][p] for o in offsets]) for p in (0, 1)])

    def in_order(self, offsets, members):
        start = self.row_part(offsets[0])
        if len(members) == 1:
            return members[0]
        if len(members) == 2:
            swap = start != 0
            return jnp.concatenate(
                [jnp.where(swap, members[1], members[0]), jnp.where(swap, members[0], members[1])], 0
            )
        twice = jnp.concatenate(members + members, 0)
        skip = lax.rem(self.parts - start, self.parts) * self.rows
        return lax.dynamic_slice_in_dim(twice, skip, self.parts * self.rows, 0)


def swap(value, bit, size):
    return lax.ppermute(value, "gy", [(k, k ^ bit) for k in range(size)])


def gather_rows(value, size):
    index = lax.axis_index("gy")
    kinds, rows, n = value.shape
    value = value[:, None]
    bit = size // 2
    while bit:
        other = swap(value, bit, size)
        high = (index // bit) % 2 == 1
        value = jnp.stack([jnp.where(high, other, value), jnp.where(high, value, other)], 2)
        value = value.reshape((kinds, -1, rows, n))
        bit //= 2
    return value.reshape((kinds, size * rows, n))


def scatter_rows(value, size):
    index = lax.axis_index("gy")
    kinds, rows, n = value.shape
    value = value.reshape((kinds, size, rows // size, n))
    bit = 1
    while bit < size:
        value = value.reshape((kinds, -1, 2, rows // size, n))
        mine = (index // bit) % 2
        keep = lax.dynamic_index_in_dim(value, mine, 2, False)
        give = lax.dynamic_index_in_dim(value, 1 - mine, 2, False)
        if bit > 1:
            give = give.astype(BF16)
        value = keep + swap(give, bit, size).astype(F32)
        bit *= 2
    return value[:, 0]


def build(mesh):
    gx, gy = mesh.shape["gx"], mesh.shape["gy"]

    def body(tokens, target, w_gate, w_up, w_down, t_gate, t_up, t_down):
        count = tokens.shape[0] * gy
        scale = 1.0 / math.sqrt(count)
        ring = Ring(gx, count, w_gate.shape[1])
        xfull = gather_rows(tokens[None], gy)[0]
        xturn = lax.optimization_barrier(xfull.T)

        up_parts = {}

        def up_part(part):
            if part not in up_parts:
                at = ring.column(part) * ring.width
                up_parts[part] = lax.optimization_barrier(
                    tuple(
                        matmul(xfull, lax.dynamic_slice_in_dim(w, at, ring.width, 1))
                        for w in (w_gate, w_up, t_gate, t_up)
                    )
                )
            return up_parts[part]

        def up_own(offset, piece):
            four = up_part(offset % ring.cols)
            pair = four[2 * piece : 2 * piece + 2]
            return jnp.stack([ring.rows_of(one, offset) for one in pair])

        (gate, upper), (gate_dot, upper_dot) = ring.reduce_scatter(up_own)
        silu_val, first, second = silu_parts(gate)
        hidden = (silu_val * upper).astype(BF16)
        hidden_dot = (first * gate_dot * upper + silu_val * upper_dot).astype(BF16)

        outs = []
        hid_parts = {}

        def down(part, pieces):
            at = ring.column(part) * ring.width
            w = lax.dynamic_slice_in_dim(w_down, at, ring.width, 0)
            t = lax.dynamic_slice_in_dim(t_down, at, ring.width, 0)
            hid, hid_dot = pieces
            hid_parts[part] = pieces
            terms = (matmul(hid, w), matmul(hid_dot, w) + matmul(hid, t))
            outs[:] = [a + b for a, b in zip(outs, terms)] if outs else terms

        ring.all_gather([hidden, hidden_dot], down)
        output, output_dot = scatter_rows(jnp.stack(outs), gy)
        grad = ((output - target.astype(F32)) * scale).astype(BF16)
        grad_dot = (output_dot * scale).astype(BF16)
        grad_full, grad_dot_full = gather_rows(jnp.stack([grad, grad_dot]), gy)

        back_parts = {}

        def back_own(offset, piece):
            part = offset % ring.cols
            if part not in back_parts:
                at = ring.column(part) * ring.width
                w = lax.dynamic_slice_in_dim(w_down, at, ring.width, 0)
                t = lax.dynamic_slice_in_dim(t_down, at, ring.width, 0)
                back_parts[part] = lax.optimization_barrier(
                    (tail_dot(grad_full, w), tail_dot(grad_dot_full, w) + tail_dot(grad_full, t))
                )
            return ring.rows_of(back_parts[part][piece], offset)

        back, back_dot = ring.reduce_scatter(back_own)
        hvp_down = jnp.zeros(w_down.shape, BF16)
        for part, (hid, hid_dot) in hid_parts.items():
            term = (lead_dot(hid_dot, grad_full) + lead_dot(hid, grad_dot_full)).astype(BF16)
            hvp_down = lax.dynamic_update_slice_in_dim(
                hvp_down, term, ring.column(part) * ring.width, 0
            )
        gate_in = (
            back_dot * upper * first + back * upper_dot * first + back * upper * second * gate_dot
        ).astype(BF16)
        upper_in = (back_dot * silu_val + back * first * gate_dot).astype(BF16)

        hvps = [jnp.zeros(w_gate.shape, BF16), jnp.zeros(w_up.shape, BF16)]

        def weigh(part, pieces):
            at = ring.column(part) * ring.width
            for k in (0, 1):
                term = matmul(xturn, pieces[k]).astype(BF16)
                hvps[k] = lax.dynamic_update_slice_in_dim(hvps[k], term, at, 1)

        ring.all_gather([gate_in, upper_in], weigh)
        return (hvps[0], hvps[1], hvp_down)

    return body


def solution(mesh):
    return jax.shard_map(
        build(mesh),
        mesh=mesh,
        in_specs=(
            P("gy", "gx"),
            P("gy", "gx"),
            P("gx", "gy"),
            P("gx", "gy"),
            P("gy", "gx"),
            P("gx", "gy"),
            P("gx", "gy"),
            P("gy", "gx"),
        ),
        out_specs=(P("gx", "gy"), P("gx", "gy"), P("gy", "gx")),
        check_vma=False,
    )
```

```python
import math

import jax
import jax.numpy as jnp
from jax import lax
from jax.experimental import pallas as pl
from jax.experimental.pallas import tpu as pltpu
from jax.sharding import PartitionSpec as P


LANES = 128
BF16 = jnp.bfloat16
F32 = jnp.float32
LEAD = (1, -1)
HOLD = 1
OUTER = 256


def silu_parts(gate):
    sig = jax.nn.sigmoid(gate)
    first = sig * (1.0 + gate * (1.0 - sig))
    second = sig * (1.0 - sig) * (2.0 + gate * (1.0 - 2.0 * sig))
    return (gate * sig, first, second)


def matmul(left, right):
    return jnp.dot(left, right, preferred_element_type=F32)


def lead_dot(left, right):
    return lax.dot_general(left, right, (((0,), (0,)), ((), ())), preferred_element_type=F32)


def tail_dot(left, right):
    return lax.dot_general(left, right, (((1,), (1,)), ((), ())), preferred_element_type=F32)


def after(value, *others):
    return lax.optimization_barrier((value,) + others)[0]


def modulo(value, size):
    return value & (size - 1) if size & (size - 1) == 0 else lax.rem(value, size)


class Ring:
    def __init__(self, size, tokens, width):
        self.size = size
        self.half = size // 2
        order = list(range(0, size, 2)) + list(range(size - 1, 0, -2))
        self.ahead = [(order[k], order[(k + 1) % size]) for k in range(size)]
        self.back = [(b, a) for a, b in self.ahead]
        index = lax.axis_index("gx").astype(jnp.int32)
        self.pos = jnp.where((index & 1) == 0, index >> 1, size - 1 - (index >> 1))
        self.cols = column_parts(size, width)
        self.parts = size // self.cols
        self.rows = tokens // self.parts
        self.width = width // self.cols
        at = [modulo(self.pos + k, size) for k in range(size)]
        self.row_parts = [lax.div(place, self.cols) if self.cols & (self.cols - 1) else place >> (self.cols.bit_length() - 1) for place in at]
        self.columns = [modulo(self.pos + k, self.cols) for k in range(self.cols)]

    def column_index(self, offset):
        return self.columns[offset % self.cols]

    def column(self, offset):
        return self.column_index(offset) * self.width

    def row_part(self, offset):
        return self.row_parts[offset % self.size]

    def rows_of(self, array, offset):
        return lax.dynamic_slice_in_dim(array, self.row_part(offset) * self.rows, self.rows, 0)

    def send(self, value, way):
        return lax.ppermute(value, "gx", self.ahead if way == 1 else self.back)

    def ways(self, far, lead):
        return (lead,) if far == self.half else (lead, -lead)

    def reduce_all(self, owns):
        flying = ({}, {})
        last = None
        for turn in range(self.half):
            for piece in (0, 1):
                for far, way in (
                    (self.half - turn, LEAD[piece]),
                    (self.half - turn - 1, -LEAD[piece]),
                ):
                    if far == 0:
                        continue
                    value = owns[piece](way * far)
                    if way in flying[piece]:
                        value = value + after(flying[piece][way], last).astype(F32)
                    last = value.astype(BF16)
                    flying[piece][way] = self.send(last, way)
        return [self.reduce_end(owns[piece], flying[piece]) for piece in (0, 1)]

    def reduce_end(self, own, flying):
        return own(0) + flying[1].astype(F32) + flying[-1].astype(F32)

    def gather_step(self, held, far, lead, hold=None):
        for way in self.ways(far, lead):
            value = held[-way * (far - 1)]
            if hold is not None:
                value = after(value, hold)
            held[self.half if far == self.half else -way * far] = self.send(value, way)

    def ready(self, held, done):
        for part in range(self.cols):
            offsets = [o for o in range(1 - self.half, self.half + 1) if (o - part) % self.cols == 0]
            if part not in done and all(o in held for o in offsets):
                done.add(part)
                yield part, self.in_order(offsets, [held[o] for o in offsets])

    def in_order(self, offsets, members):
        start = self.row_part(offsets[0])
        if len(members) == 1:
            return members[0]
        if len(members) == 2:
            swap = start != 0
            return jnp.concatenate(
                [jnp.where(swap, members[1], members[0]), jnp.where(swap, members[0], members[1])], 0
            )
        twice = jnp.concatenate(members + members, 0)
        skip = modulo(self.parts - start, self.parts) * self.rows
        return lax.dynamic_slice_in_dim(twice, skip, self.parts * self.rows, 0)


def column_parts(size, width):
    return max(c for c in range(1, size) if size % c == 0 and width % (c * LANES) == 0)


def outer_kernel(at_ref, left_ref, right_ref, *rest):
    rest[-1][...] = lead_dot(left_ref[...], right_ref[...]).astype(BF16)


def outer(at, blocks, left, right, before):
    count, depth = left.shape
    width = right.shape[1]
    tile = math.gcd(depth, OUTER)
    return pl.pallas_call(
        outer_kernel,
        out_shape=jax.ShapeDtypeStruct((depth, width), BF16),
        grid_spec=pltpu.PrefetchScalarGridSpec(
            num_scalar_prefetch=1,
            grid=(blocks,),
            in_specs=[
                pl.BlockSpec((count, tile), lambda i, at: (0, at[0] + i)),
                pl.BlockSpec((count, width), lambda i, at: (0, 0)),
            ]
            + [pl.BlockSpec(memory_space=pl.ANY)] * len(before),
            out_specs=pl.BlockSpec((tile, width), lambda i, at: (at[0] + i, 0)),
        ),
        input_output_aliases={3: 0} if before else {},
        compiler_params=pltpu.CompilerParams(vmem_limit_bytes=16 * 2**20),
        cost_estimate=pl.CostEstimate(
            flops=2 * blocks * tile * count * width,
            bytes_accessed=2 * blocks * tile * width,
            transcendentals=0,
        ),
        name="outer",
    )(jnp.full((1,), at, jnp.int32), left, right, *before)


def tail_kernel(at_ref, x_ref, gate_ref, up_ref, *rest):
    hvp_gate, hvp_up = rest[-2:]
    hvp_gate[...] = matmul(x_ref[...], gate_ref[...]).astype(BF16)
    hvp_up[...] = matmul(x_ref[...], up_ref[...]).astype(BF16)


def tail(at, xturn, gate, up, before, shape):
    depth, count = xturn.shape
    width = gate.shape[1]
    tile = math.gcd(depth, 256)
    whole = pl.BlockSpec((count, width), lambda i, at: (0, 0))
    out = pl.BlockSpec((tile, width), lambda i, at: (i, at[0]))
    place = pl.BlockSpec(memory_space=pl.ANY)
    return pl.pallas_call(
        tail_kernel,
        out_shape=[jax.ShapeDtypeStruct(shape, BF16)] * 2,
        grid_spec=pltpu.PrefetchScalarGridSpec(
            num_scalar_prefetch=1,
            grid=(depth // tile,),
            in_specs=[pl.BlockSpec((tile, count), lambda i, at: (i, 0)), whole, whole]
            + [place] * len(before),
            out_specs=[out, out],
        ),
        input_output_aliases={4 + k: k for k in range(len(before))},
        compiler_params=pltpu.CompilerParams(vmem_limit_bytes=24 * 2**20),
        cost_estimate=pl.CostEstimate(
            flops=4 * depth * count * width, bytes_accessed=4 * depth * width, transcendentals=0
        ),
        name="tail",
    )(at.reshape((1,)).astype(jnp.int32), xturn, gate, up, *before)


def swap(value, bit, size):
    return lax.ppermute(value, "gy", [(k, k ^ bit) for k in range(size)])


def gather_rows(value, size):
    index = lax.axis_index("gy").astype(jnp.int32)
    kinds, rows, n = value.shape
    value = value[:, None]
    bit = size // 2
    while bit:
        other = swap(value, bit, size)
        high = (index & bit) != 0
        value = jnp.stack([jnp.where(high, other, value), jnp.where(high, value, other)], 2)
        value = value.reshape((kinds, -1, rows, n))
        bit //= 2
    return value.reshape((kinds, size * rows, n))


def scatter_rows(value, size):
    index = lax.axis_index("gy").astype(jnp.int32)
    kinds, rows, n = value.shape
    value = value.reshape((kinds, size, rows // size, n))
    bit = 1
    while bit < size:
        value = value.reshape((kinds, -1, 2, rows // size, n))
        mine = jnp.where((index & bit) != 0, 1, 0)
        keep = lax.dynamic_index_in_dim(value, mine, 2, False)
        give = lax.dynamic_index_in_dim(value, 1 - mine, 2, False)
        if bit > 1:
            give = give.astype(BF16)
        value = keep + swap(give, bit, size)
        bit *= 2
    return value[:, 0]


def build(mesh):
    gx, gy = mesh.shape["gx"], mesh.shape["gy"]

    def body(tokens, target, w_gate, w_up, w_down, t_gate, t_up, t_down):
        count = tokens.shape[0] * gy
        scale = 1.0 / math.sqrt(count)
        ring = Ring(gx, count, w_gate.shape[1])
        half = ring.half
        xfull = gather_rows(tokens[None], gy)[0]
        xturn = lax.optimization_barrier(xfull.T)
        up_parts = {}

        def up_own(piece):
            def own(offset):
                part = offset % ring.cols
                if (part, piece) not in up_parts:
                    at = ring.column(part)
                    up_parts[part, piece] = lax.optimization_barrier(
                        tuple(
                            matmul(xfull, lax.dynamic_slice_in_dim(w, at, ring.width, 1))
                            for w in ((w_gate, w_up), (t_gate, t_up))[piece]
                        )
                    )
                return jnp.stack([ring.rows_of(one, offset) for one in up_parts[part, piece]])

            return own

        (gate, upper), (gate_dot, upper_dot) = ring.reduce_all([up_own(0), up_own(1)])
        silu_val, first, second = silu_parts(gate)
        hidden = (silu_val * upper).astype(BF16)
        hidden_dot = (first * gate_dot * upper + silu_val * upper_dot).astype(BF16)

        held = [{0: hidden}, {0: hidden_dot}]
        done = [set(), set()]
        hid_parts = [{}, {}]
        outs = list(lax.optimization_barrier([jnp.zeros((count, w_down.shape[1]), F32)] * 2))

        def down(piece):
            for part, rows in ring.ready(held[piece], done[piece]):
                hid_parts[piece][part] = rows
                at = ring.column(part)
                total = outs[piece]
                total = total + matmul(rows, lax.dynamic_slice_in_dim(w_down, at, ring.width, 0))
                if piece:
                    t = lax.dynamic_slice_in_dim(t_down, at, ring.width, 0)
                    total = total + matmul(hid_parts[0][part], t)
                outs[piece] = total

        hold = None
        for piece in (0, 1):
            for far in range(1, half + 1):
                ring.gather_step(held[piece], far, LEAD[piece], hold if far == 1 else None)
                down(piece)
            hold = held[0][LEAD[0] * -min(HOLD, half - 1)]

        grads, backs = [None, None], [None, None]
        back_parts = {}

        def back_own(piece):
            def own(offset):
                part = offset % ring.cols
                if (part, piece) not in back_parts:
                    at = ring.column(part)
                    w = lax.dynamic_slice_in_dim(w_down, at, ring.width, 0)
                    term = tail_dot(grads[piece], w)
                    if piece:
                        t = lax.dynamic_slice_in_dim(t_down, at, ring.width, 0)
                        term = term + tail_dot(grads[0], t)
                    back_parts[part, piece] = lax.optimization_barrier(term)
                return ring.rows_of(back_parts[part, piece], offset)

            return own

        for piece in (0, 1):
            total = scatter_rows(outs[piece][None], gy)[0]
            if piece == 0:
                total = total - target.astype(F32)
            grads[piece] = gather_rows((total * scale).astype(BF16)[None], gy)[0]
        backs = ring.reduce_all([back_own(0), back_own(1)])

        stacked = jnp.zeros((2 * count, w_down.shape[0]), BF16)
        for piece in (0, 1):
            for part, rows in hid_parts[piece].items():
                stacked = lax.dynamic_update_slice(
                    stacked, rows, ((1 - piece) * count, ring.column(part))
                )
        both = jnp.concatenate((grads[0], grads[1]), 0)
        steps = w_down.shape[0] // math.gcd(w_down.shape[0], OUTER)
        cut = steps // 2
        hvp_down = None
        for start, stop in ((0, cut), (cut, steps)):
            if stop > start:
                hvp_down = outer(
                    start, stop - start, stacked, both, [] if hvp_down is None else [hvp_down]
                )

        back, back_dot = backs
        gate_in = (
            back_dot * upper * first + back * upper_dot * first + back * upper * second * gate_dot
        ).astype(BF16)
        upper_in = (back_dot * silu_val + back * first * gate_dot).astype(BF16)
        held = [{0: gate_in}, {0: upper_in}]
        done = [set(), set()]
        hvps = []
        for far in range(1, half + 1):
            for piece in (0, 1):
                ring.gather_step(held[piece], far, LEAD[piece])
            gates = dict(ring.ready(held[0], done[0]))
            ups = dict(ring.ready(held[1], done[1]))
            for part in gates:
                hvps = tail(
                    ring.column_index(part), xturn, gates[part], ups[part], hvps, w_gate.shape
                )
        return (hvps[0], hvps[1], hvp_down)

    return body


def solution(mesh):
    return jax.shard_map(
        build(mesh),
        mesh=mesh,
        in_specs=(
            P("gy", "gx"),
            P("gy", "gx"),
            P("gx", "gy"),
            P("gx", "gy"),
            P("gy", "gx"),
            P("gx", "gy"),
            P("gx", "gy"),
            P("gy", "gx"),
        ),
        out_specs=(P("gx", "gy"), P("gx", "gy"), P("gy", "gx")),
        check_vma=False,
    )
```

```python
import math

import jax
import jax.numpy as jnp
from jax import lax
from jax.experimental import pallas as pl
from jax.experimental.pallas import tpu as pltpu
from jax.sharding import PartitionSpec as P


LANES = 128
BF16 = jnp.bfloat16
F32 = jnp.float32
LEAD = (1, -1)
CHUNKS = 2
OUTER = 256


def silu_parts(gate):
    sig = jax.nn.sigmoid(gate)
    first = sig * (1.0 + gate * (1.0 - sig))
    second = sig * (1.0 - sig) * (2.0 + gate * (1.0 - 2.0 * sig))
    return (gate * sig, first, second)


def matmul(left, right):
    return jnp.dot(left, right, preferred_element_type=F32)


def lead_dot(left, right):
    return lax.dot_general(left, right, (((0,), (0,)), ((), ())), preferred_element_type=F32)


def tail_dot(left, right):
    return lax.dot_general(left, right, (((1,), (1,)), ((), ())), preferred_element_type=F32)


def after(value, *others):
    return lax.optimization_barrier((value,) + others)[0]


def modulo(value, size):
    return value & (size - 1) if size & (size - 1) == 0 else lax.rem(value, size)


class Ring:
    def __init__(self, size, tokens, width):
        self.size = size
        self.half = size // 2
        order = list(range(0, size, 2)) + list(range(size - 1, 0, -2))
        self.ahead = [(order[k], order[(k + 1) % size]) for k in range(size)]
        self.back = [(b, a) for a, b in self.ahead]
        index = lax.axis_index("gx").astype(jnp.int32)
        self.pos = jnp.where((index & 1) == 0, index >> 1, size - 1 - (index >> 1))
        self.cols = column_parts(size, width)
        self.parts = size // self.cols
        self.rows = tokens // self.parts
        self.width = width // self.cols
        at = [modulo(self.pos + k, size) for k in range(size)]
        self.row_parts = [lax.div(place, self.cols) if self.cols & (self.cols - 1) else place >> (self.cols.bit_length() - 1) for place in at]
        self.columns = [modulo(self.pos + k, self.cols) for k in range(self.cols)]

    def column_index(self, offset):
        return self.columns[offset % self.cols]

    def column(self, offset):
        return self.column_index(offset) * self.width

    def row_part(self, offset):
        return self.row_parts[offset % self.size]

    def rows_of(self, array, offset):
        return lax.dynamic_slice_in_dim(array, self.row_part(offset) * self.rows, self.rows, 0)

    def send(self, value, way):
        return lax.ppermute(value, "gx", self.ahead if way == 1 else self.back)

    def ways(self, far, lead):
        return (lead,) if far == self.half else (lead, -lead)

    def reduce_all(self, owns, early=False):
        flying = ({}, {})
        last = None
        turns = [
            (piece, self.half - turn - late, LEAD[piece] * (-1 if late else 1))
            for turn in range(self.half)
            for piece in (0, 1)
            for late in (0, 1)
            if turn + late < self.half
        ]
        if early:
            turns[3:5] = turns[4:2:-1]
        for piece, far, way in turns:
            value = owns[piece](way * far)
            if way in flying[piece]:
                value = value + after(flying[piece][way], last).astype(F32)
            last = value.astype(BF16)
            flying[piece][way] = self.send(last, way)
        return [self.reduce_end(owns[piece], flying[piece]) for piece in (0, 1)]

    def reduce_end(self, own, flying):
        return own(0) + flying[1].astype(F32) + flying[-1].astype(F32)

    def gather_step(self, held, far, lead):
        for way in self.ways(far, lead):
            value = held[-way * (far - 1)]
            held[self.half if far == self.half else -way * far] = self.send(value, way)

    def ready(self, held, done):
        for part in range(self.cols):
            offsets = [o for o in range(1 - self.half, self.half + 1) if (o - part) % self.cols == 0]
            if part not in done and all(o in held for o in offsets):
                done.add(part)
                yield part, self.in_order(offsets, [held[o] for o in offsets])

    def in_order(self, offsets, members):
        start = self.row_part(offsets[0])
        if len(members) == 1:
            return members[0]
        if len(members) == 2:
            swap = start != 0
            return jnp.concatenate(
                [jnp.where(swap, members[1], members[0]), jnp.where(swap, members[0], members[1])], 0
            )
        twice = jnp.concatenate(members + members, 0)
        skip = modulo(self.parts - start, self.parts) * self.rows
        return lax.dynamic_slice_in_dim(twice, skip, self.parts * self.rows, 0)


def column_parts(size, width):
    return max(c for c in range(1, size) if size % c == 0 and width % (c * LANES) == 0)


def wide_kernel(at_ref, x_ref, first_ref, second_ref, out_ref):
    both = matmul(x_ref[...], jnp.concatenate([first_ref[...], second_ref[...]], 1))
    out_ref[0, 0] = both[:, :LANES]
    out_ref[0, 1] = both[:, LANES:]


def wide(columns, x, first, second, width):
    count, depth = x.shape
    parts = len(columns)
    tiles = width // LANES
    weight = pl.BlockSpec(
        (depth, LANES), lambda i, at: (0, at[lax.div(i, tiles)] * tiles + lax.rem(i, tiles))
    )
    return pl.pallas_call(
        wide_kernel,
        out_shape=jax.ShapeDtypeStruct((parts, 2, count, width), F32),
        grid_spec=pltpu.PrefetchScalarGridSpec(
            num_scalar_prefetch=1,
            grid=(parts * tiles,),
            in_specs=[pl.BlockSpec((count, depth), lambda i, at: (0, 0)), weight, weight],
            out_specs=pl.BlockSpec(
                (1, 2, count, LANES),
                lambda i, at: (lax.div(i, tiles), 0, 0, lax.rem(i, tiles)),
            ),
        ),
        compiler_params=pltpu.CompilerParams(vmem_limit_bytes=8 * 2**20),
        cost_estimate=pl.CostEstimate(
            flops=4 * count * depth * width * parts,
            bytes_accessed=4 * depth * width * parts,
            transcendentals=0,
        ),
        name="wide",
    )(jnp.stack(columns).astype(jnp.int32), x, first, second)


def outer_kernel(at_ref, left_ref, right_ref, *rest):
    rest[-1][...] = lead_dot(left_ref[...], right_ref[...]).astype(BF16)


def outer(at, blocks, left, right, before):
    count, depth = left.shape
    width = right.shape[1]
    tile = math.gcd(depth, OUTER)
    return pl.pallas_call(
        outer_kernel,
        out_shape=jax.ShapeDtypeStruct((depth, width), BF16),
        grid_spec=pltpu.PrefetchScalarGridSpec(
            num_scalar_prefetch=1,
            grid=(blocks,),
            in_specs=[
                pl.BlockSpec((count, tile), lambda i, at: (0, at[0] + i)),
                pl.BlockSpec((count, width), lambda i, at: (0, 0)),
            ]
            + [pl.BlockSpec(memory_space=pl.ANY)] * len(before),
            out_specs=pl.BlockSpec((tile, width), lambda i, at: (at[0] + i, 0)),
        ),
        input_output_aliases={3: 0} if before else {},
        compiler_params=pltpu.CompilerParams(vmem_limit_bytes=6 * 2**20),
        cost_estimate=pl.CostEstimate(
            flops=2 * blocks * tile * count * width,
            bytes_accessed=2 * blocks * tile * width,
            transcendentals=0,
        ),
        name="outer",
    )(jnp.full((1,), at, jnp.int32), left, right, *before)


def tail_kernel(at_ref, x_ref, gate_ref, up_ref, *rest):
    hvp_gate, hvp_up = rest[-2:]
    hvp_gate[...] = matmul(x_ref[...], gate_ref[...]).astype(BF16)
    hvp_up[...] = matmul(x_ref[...], up_ref[...]).astype(BF16)


def tail(at, xturn, gate, up, before, shape):
    depth, count = xturn.shape
    width = gate.shape[1]
    tile = math.gcd(depth, 256)
    whole = pl.BlockSpec((count, width), lambda i, at: (0, 0))
    out = pl.BlockSpec((tile, width), lambda i, at: (i, at[0]))
    place = pl.BlockSpec(memory_space=pl.ANY)
    return pl.pallas_call(
        tail_kernel,
        out_shape=[jax.ShapeDtypeStruct(shape, BF16)] * 2,
        grid_spec=pltpu.PrefetchScalarGridSpec(
            num_scalar_prefetch=1,
            grid=(depth // tile,),
            in_specs=[pl.BlockSpec((tile, count), lambda i, at: (i, 0)), whole, whole]
            + [place] * len(before),
            out_specs=[out, out],
        ),
        input_output_aliases={4 + k: k for k in range(len(before))},
        compiler_params=pltpu.CompilerParams(vmem_limit_bytes=8 * 2**20),
        cost_estimate=pl.CostEstimate(
            flops=4 * depth * count * width, bytes_accessed=4 * depth * width, transcendentals=0
        ),
        name="tail",
    )(at.reshape((1,)).astype(jnp.int32), xturn, gate, up, *before)


def swap(value, bit, size):
    return lax.ppermute(value, "gy", [(k, k ^ bit) for k in range(size)])


def gather_rows(value, size):
    index = lax.axis_index("gy").astype(jnp.int32)
    kinds, rows, n = value.shape
    value = value[:, None]
    bit = size // 2
    while bit:
        other = swap(value, bit, size)
        high = (index & bit) != 0
        value = jnp.stack([jnp.where(high, other, value), jnp.where(high, value, other)], 2)
        value = value.reshape((kinds, -1, rows, n))
        bit //= 2
    return value.reshape((kinds, size * rows, n))


def scatter_rows(value, size):
    index = lax.axis_index("gy").astype(jnp.int32)
    kinds, rows, n = value.shape
    value = value.reshape((kinds, size, rows // size, n))
    bit = 1
    while bit < size:
        value = value.reshape((kinds, -1, 2, rows // size, n))
        mine = jnp.where((index & bit) != 0, 1, 0)
        keep = lax.dynamic_index_in_dim(value, mine, 2, False)
        give = lax.dynamic_index_in_dim(value, 1 - mine, 2, False)
        if bit > 1:
            give = give.astype(BF16)
        value = keep + swap(give, bit, size)
        bit *= 2
    return value[:, 0]


def build(mesh):
    gx, gy = mesh.shape["gx"], mesh.shape["gy"]

    def body(tokens, target, w_gate, w_up, w_down, t_gate, t_up, t_down):
        count = tokens.shape[0] * gy
        scale = 1.0 / math.sqrt(count)
        ring = Ring(gx, count, w_gate.shape[1])
        half = ring.half
        xfull = gather_rows(tokens[None], gy)[0]
        xturn = lax.optimization_barrier(xfull.T)
        up_parts = {}

        tangents = {}
        for parts in ([3, 1, 2] if ring.cols == 4 else list(range(1, ring.cols)),):
            if parts:
                both = wide(
                    [ring.column_index(part) for part in parts], xfull, t_gate, t_up, ring.width
                )
                tangents.update({part: (both, place) for place, part in enumerate(parts)})

        def up_own(piece):
            def own(offset):
                part = offset % ring.cols
                if piece and part in tangents:
                    both, place = tangents[part]
                    start = ring.row_part(offset) * ring.rows
                    return lax.dynamic_slice_in_dim(both[place], start, ring.rows, 1)
                if (part, piece) not in up_parts:
                    at = ring.column(part)
                    up_parts[part, piece] = lax.optimization_barrier(
                        tuple(
                            matmul(xfull, lax.dynamic_slice_in_dim(w, at, ring.width, 1))
                            for w in ((w_gate, w_up), (t_gate, t_up))[piece]
                        )
                    )
                return jnp.stack([ring.rows_of(one, offset) for one in up_parts[part, piece]])

            return own

        (gate, upper), (gate_dot, upper_dot) = ring.reduce_all([up_own(0), up_own(1)], True)
        silu_val, first, second = silu_parts(gate)
        hidden = (silu_val * upper).astype(BF16)
        hidden_dot = (first * gate_dot * upper + silu_val * upper_dot).astype(BF16)

        held = [{0: hidden}, {0: hidden_dot}]
        done = [set(), set()]
        hid_parts = [{}, {}]
        outs = list(lax.optimization_barrier([jnp.zeros((count, w_down.shape[1]), F32)] * 2))

        def down(piece):
            for part, rows in ring.ready(held[piece], done[piece]):
                hid_parts[piece][part] = rows
                at = ring.column(part)
                total = outs[piece]
                total = total + matmul(rows, lax.dynamic_slice_in_dim(w_down, at, ring.width, 0))
                if piece:
                    t = lax.dynamic_slice_in_dim(t_down, at, ring.width, 0)
                    total = total + matmul(hid_parts[0][part], t)
                outs[piece] = total

        for far in range(1, half + 1):
            for piece in (0, 1):
                ring.gather_step(held[piece], far, LEAD[piece])
                down(piece)

        grads, backs = [None, None], [None, None]
        back_parts = {}

        def back_own(piece):
            def own(offset):
                part = offset % ring.cols
                if (part, piece) not in back_parts:
                    at = ring.column(part)
                    w = lax.dynamic_slice_in_dim(w_down, at, ring.width, 0)
                    term = tail_dot(grads[piece], w)
                    if piece:
                        t = lax.dynamic_slice_in_dim(t_down, at, ring.width, 0)
                        term = term + tail_dot(grads[0], t)
                    back_parts[part, piece] = lax.optimization_barrier(term)
                return ring.rows_of(back_parts[part, piece], offset)

            return own

        for piece in (0, 1):
            total = scatter_rows(outs[piece][None], gy)[0]
            if piece == 0:
                total = total - target.astype(F32)
            grads[piece] = gather_rows((total * scale).astype(BF16)[None], gy)[0]
        backs = ring.reduce_all([back_own(0), back_own(1)])

        stacked = jnp.zeros((2 * count, w_down.shape[0]), BF16)
        for piece in (0, 1):
            for part, rows in hid_parts[piece].items():
                stacked = lax.dynamic_update_slice(
                    stacked, rows, ((1 - piece) * count, ring.column(part))
                )
        both = jnp.concatenate((grads[0], grads[1]), 0)
        steps = w_down.shape[0] // math.gcd(w_down.shape[0], OUTER)
        cuts = [-(-steps * k // CHUNKS) for k in range(CHUNKS + 1)]
        hvp_down = None
        for start, stop in zip(cuts, cuts[1:]):
            if stop > start:
                hvp_down = outer(
                    start, stop - start, stacked, both, [] if hvp_down is None else [hvp_down]
                )

        back, back_dot = backs
        gate_in = (
            back_dot * upper * first + back * upper_dot * first + back * upper * second * gate_dot
        ).astype(BF16)
        upper_in = (back_dot * silu_val + back * first * gate_dot).astype(BF16)
        held = [{0: gate_in}, {0: upper_in}]
        done = [set(), set()]
        hvps = []
        for far in range(1, half + 1):
            for piece in (0, 1):
                ring.gather_step(held[piece], far, LEAD[piece])
            gates = dict(ring.ready(held[0], done[0]))
            ups = dict(ring.ready(held[1], done[1]))
            for part in gates:
                hvps = tail(
                    ring.column_index(part), xturn, gates[part], ups[part], hvps, w_gate.shape
                )
        return (hvps[0], hvps[1], hvp_down)

    return body


def solution(mesh):
    return jax.shard_map(
        build(mesh),
        mesh=mesh,
        in_specs=(
            P("gy", "gx"),
            P("gy", "gx"),
            P("gx", "gy"),
            P("gx", "gy"),
            P("gy", "gx"),
            P("gx", "gy"),
            P("gx", "gy"),
            P("gy", "gx"),
        ),
        out_specs=(P("gx", "gy"), P("gx", "gy"), P("gy", "gx")),
        check_vma=False,
    )
```
